32 devices in a mesh: gx: 4 (over y, x), gy: 4 (over z), gz: 2 (over core).
Axes of the slice: x: 2, y: 2, z: 4, core: 2. Of those that a mesh axis runs over, the one named last changes fastest.
Arguments:
- residual: float32 [3, 32, 256, 512], P(None, 'gz', 'gx', 'gy'), may hold values from -32 to 32
- edge_diag: float32 [3, 32, 256, 512], P(None, 'gz', 'gx', 'gy'), may hold values from 6.5 to 9
- node_shift: float32 [32, 256, 512], P('gz', 'gx', 'gy'), may hold values from 0.05 to 3
- coarse_shift: float32 [16, 128, 256], P('gz', 'gx', 'gy'), may hold values from 0.05 to 3
Outputs:
- correction: float32 [3, 32, 256, 512], P(None, 'gz', 'gx', 'gy')
The draws below stay inside these ranges and needn't reach their ends.
All inputs are finite; a program needn't handle non-finite values.
Results may differ from the reference program's by a relative error of at most 0.000021.
Values sent between devices are 32-bit elements; how exact they have to be, the bound alone decides.
A program may use at most 128 MiB of HBM per device.

```python
import math
import jax
import jax.numpy as jnp

NX = 256
NY = 512
NZ = 32


def draw_residual(key, part):
    second_key = jax.random.fold_in(jax.random.fold_in(key, 11), 1)
    zpos = jnp.arange(NZ, dtype=jnp.float32) / NZ
    xpos = jnp.arange(NX, dtype=jnp.float32) / NX
    ramp = 2.0 * (1.0 + zpos)[:, None, None] * (1.0 + xpos)[None, :, None] * jnp.ones((1, 1, NY), jnp.float32)
    rough = jnp.clip(jax.random.normal(second_key, (3, NZ, NX, NY), jnp.float32), -4.0, 4.0)
    values = ramp[None] * rough
    return values.astype(jnp.float32)


def level_of(own_key, shape, shards, least, top_value):
    loudness = 1.0
    for position, shards_of in shards:
        draws = jax.random.uniform(jax.random.fold_in(jax.random.fold_in(own_key, 6), position), (shards_of,), jnp.float32, least / len(shards), top_value / len(shards))
        loudness = loudness * jnp.repeat(jnp.exp(draws), shape[position] // shards_of).reshape((-1,) + (1,) * (len(shape) - 1 - position))
    return loudness


def setup_inputs(seed: int = 0) -> dict:
    keys = jax.random.split(jax.random.key(seed), 5)
    return {
        "residual": draw_residual(jax.random.fold_in(keys[4], 71), 0),
        "edge_diag": jnp.clip(6.5 + 2.5 * jax.random.uniform(keys[1], (3, NZ, NX, NY), jnp.float32) ** level_of(keys[1], (3, NZ, NX, NY), ((1, 2), (2, 4), (3, 4)), -0.2, 0.2), 6.5, 9.0),
        "node_shift": jnp.clip(jnp.exp(math.log(3.0) - 4.0943445 * jax.random.uniform(keys[2], (NZ, NX, NY), jnp.float32) ** level_of(keys[2], (NZ, NX, NY), ((0, 2), (1, 4), (2, 4)), -0.2, 0.2)), 0.05, 3.0),
        "coarse_shift": jnp.clip(jnp.exp(math.log(3.0) - 4.0943445 * jax.random.uniform(keys[3], (NZ // 2, NX // 2, NY // 2), jnp.float32) ** level_of(keys[3], (NZ // 2, NX // 2, NY // 2), ((0, 2), (1, 4), (2, 4)), -0.2, 0.2)), 0.05, 3.0),
    }


def neighbours(padded):
    total = padded[2:, 1:-1, 1:-1] + padded[:-2, 1:-1, 1:-1]
    total = total + padded[1:-1, 2:, 1:-1] + padded[1:-1, :-2, 1:-1]
    return total + padded[1:-1, 1:-1, 2:] + padded[1:-1, 1:-1, :-2]


def apply_op(field, diagonal):
    return diagonal * field - neighbours(jnp.pad(field, 1))


def reference(residual, edge_diag, node_shift, coarse_shift):
    scaled = residual / edge_diag
    padded = jnp.pad(scaled, ((0, 0), (1, 1), (1, 1), (1, 1)))
    edge_near = jnp.stack([neighbours(padded[component]) for component in range(3)])
    smooth_part = 2.0 * scaled - (edge_diag * scaled - edge_near) / edge_diag
    nodal_rhs = (padded[0, :-2, 1:-1, 1:-1] - scaled[0]) + (padded[1, 1:-1, :-2, 1:-1] - scaled[1]) + (padded[2, 1:-1, 1:-1, :-2] - scaled[2])
    node_diag = 6.0 + node_shift
    first_guess = nodal_rhs / node_diag
    node_res = nodal_rhs - apply_op(first_guess, node_diag)
    sx, sy, sz = node_res.shape
    coarse_rhs = node_res.reshape(sx // 2, 2, sy // 2, 2, sz // 2, 2).sum(axis=(1, 3, 5))
    coarse_diag = 6.0 + coarse_shift
    first_dir = coarse_rhs / coarse_diag
    first_image = apply_op(first_dir, coarse_diag)
    second_dir = first_image / coarse_diag
    second_image = apply_op(second_dir, coarse_diag)
    gone = jnp.sum(first_dir * coarse_rhs)
    gtwo = jnp.sum(second_dir * coarse_rhs)
    hone = jnp.sum(first_dir * first_image)
    hmix = jnp.sum(second_dir * first_image)
    htwo = jnp.sum(second_dir * second_image)
    coef_two = (gtwo - hmix * gone / hone) / (htwo - hmix * hmix / hone)
    coef_one = (gone - hmix * coef_two) / hone
    coarse_sol = coef_one * first_dir + coef_two * second_dir
    spread = jnp.broadcast_to(coarse_sol[:, None, :, None, :, None], (sx // 2, 2, sy // 2, 2, sz // 2, 2)).reshape(sx, sy, sz)
    nodal = first_guess + spread
    final_nodal = nodal + (nodal_rhs - apply_op(nodal, node_diag)) / node_diag
    fpad = jnp.pad(final_nodal, 1)
    grads = jnp.stack([fpad[2:, 1:-1, 1:-1] - final_nodal, fpad[1:-1, 2:, 1:-1] - final_nodal, fpad[1:-1, 1:-1, 2:] - final_nodal])
    return smooth_part + grads
```

```python
import functools

import jax
import jax.numpy as jnp
from jax import lax
from jax.experimental import pallas as pl
from jax.experimental.pallas import tpu as pltpu
from jax.sharding import PartitionSpec as P

MESH = pl.DeviceIdType.MESH
AXES = ("gz", "gx", "gy")
FGI, V1I, V2I, F0I = 3, 4, 5, 6
PAD = 8


def kernel(
    sizes,
    res, dia, shf, csh, out,
    R, D, NI, CS, S, FG, CI, CR, A1, T, V1, V2, F, FN, OB,
    SX, RX, SY, RY, PZ, PX, PY,
    in_sem, out_sem, send_sem, recv_sem, psend, precv,
):
    n0, n1, n2 = NI.shape
    m0, m1, m2 = CS.shape
    groups = n1 // 8
    me = [lax.axis_index(a) for a in AXES]
    rows = pl.ds(PAD, n1)

    loads = []
    for k in (2, 1, 0):
        for src, dst in ((res, R), (dia, D)):
            loads.append(pltpu.make_async_copy(src.at[k], dst.at[k], in_sem.at[len(loads)]))
    loads.append(pltpu.make_async_copy(shf, NI, in_sem.at[6]))
    loads.append(pltpu.make_async_copy(csh, CS, in_sem.at[7]))
    for c in loads:
        c.start()

    zplane = jnp.zeros((n1, n2), jnp.float32)
    for k in range(3):
        S[k, 0, rows] = zplane
        S[k, n0 + 1, rows] = zplane
        F[k, n0] = zplane
    FG[0, rows] = zplane
    FG[n0 + 1, rows] = zplane
    for V in (V1, V2):
        V[0, rows] = zplane
        V[m0 + 1, rows] = zplane
    RX[...] = jnp.zeros(RX.shape, jnp.float32)
    RY[...] = jnp.zeros(RY.shape, jnp.float32)
    barrier = pltpu.get_barrier_semaphore()
    total = 0
    for a in range(3):
        for d in range(1, sizes[a]):
            pl.semaphore_signal(
                barrier, inc=1, device_id={AXES[a]: lax.rem(me[a] + d, sizes[a])}, device_id_type=MESH
            )
            total += 1

    lane = lax.broadcasted_iota(jnp.int32, (8, n2), 1)
    lane_full = lax.broadcasted_iota(jnp.int32, (n1, n2), 1)
    row_full = lax.broadcasted_iota(jnp.int32, (n1, n2), 0)
    keys = {p: ((lane + p // 2) // p) % (n2 // p) for p in (2, 4)}
    is_low = {p: (lane % p) >= p // 2 for p in (2, 4)}

    def place(i, g, p):
        k = i * groups + g
        per = n2 // p
        return k // per, k % per

    def pack(f, plane, count, p):
        accs = [jnp.zeros((8, n2), jnp.float32) for _ in range(place(count - 1, groups - 1, p)[0] + 1)]
        for i in range(count):
            x = plane(i)
            for g in range(groups):
                v, kk = place(i, g, p)
                part = x[8 * g : 8 * g + 8]
                if kk:
                    part = pltpu.roll(part, p * kk, 1)
                accs[v] = jnp.where(keys[p] == kk, part, accs[v])
        for v, acc in enumerate(accs):
            SY[f, v] = acc

    def arrived(f, p):
        return [jnp.where(is_low[p], RY[f, 0, v], RY[f, 1, v]) for v in range(RY.shape[2])]

    def halo(ws, i, p):
        parts = []
        for g in range(groups):
            v, kk = place(i, g, p)
            parts.append(pltpu.roll(ws[v], n2 - p * kk, 1) if kk else ws[v])
        return jnp.concatenate(parts, axis=0)

    def from_low(x, h, sh=1):
        return pltpu.roll(jnp.where(lane_full >= n2 - sh, h, x), sh, 1)

    def from_high(x, h, sh=1):
        return pltpu.roll(jnp.where(lane_full < sh, h, x), n2 - sh, 1)

    def inplane(ref, x, h, sh):
        near = ref[pl.ds(PAD - sh, n1)] + ref[pl.ds(PAD + sh, n1)]
        return near + from_low(x, h, sh) + from_high(x, h, sh)

    def field(f):
        if f < 3:
            return S.at[f], n0
        return {FGI: (FG, n0), V1I: (V1, m0), V2I: (V2, m0)}[f]

    def message(f, a, d):
        if a == 0:
            if f >= F0I:
                src, dst = F.at[f - F0I, 0], F.at[f - F0I, n0]
            else:
                ref, n = field(f)
                src = ref.at[n if d else 1, rows]
                dst = ref.at[0 if d else n + 1, rows]
        elif a == 1:
            count = m0 if f in (V1I, V2I) else n0
            src, dst = SX.at[f, d, pl.ds(0, count)], RX.at[f, 1 - d, pl.ds(0, count)]
        else:
            src, dst = SY.at[f], RY.at[f, 1 - d]
        step = 1 if d else -1
        return pltpu.make_async_remote_copy(
            src_ref=src, dst_ref=dst, send_sem=send_sem.at[f, a, d], recv_sem=recv_sem.at[f, a, d],
            device_id={AXES[a]: lax.rem(me[a] + step + sizes[a], sizes[a])}, device_id_type=MESH,
        )

    def dirs(f):
        return (0,) if f >= F0I else (0, 1)

    def can_send(a, d):
        return me[a] < sizes[a] - 1 if d else me[a] > 0

    def send(f, a):
        for d in dirs(f):
            pl.when(can_send(a, d))(lambda f=f, a=a, d=d: message(f, a, d).start())

    def receive(f, a):
        for d in dirs(f):
            pl.when(can_send(a, 1 - d))(lambda f=f, a=a, d=d: message(f, a, d).wait_recv())

    def faces_x(f, get, count):
        for i in range(count):
            SX[f, 0, i : i + 1] = get(i, 0)
            if f < F0I:
                SX[f, 1, i : i + 1] = get(i, n1 - 1)

    def rows_x(f, width):
        ref, count = field(f)
        for i in range(count):
            for w in range(width):
                ref[1 + i, PAD - 1 - w : PAD - w] = RX[f, 0, i : i + 1]
                ref[1 + i, PAD + n1 + w : PAD + n1 + w + 1] = RX[f, 1, i : i + 1]

    def exchange(f, p):
        ref, count = field(f)
        send(f, 0)
        faces_x(f, lambda i, r: ref[1 + i, PAD + r : PAD + r + 1], count)
        send(f, 1)
        pack(f, lambda i: ref[1 + i, rows], count, p)
        send(f, 2)

    for pos, k in enumerate((2, 1, 0)):
        loads[2 * pos].wait()
        loads[2 * pos + 1].wait()
        for i in range(n0):
            inv = 1.0 / D[k, i]
            D[k, i] = inv
            S[k, 1 + i, rows] = R[k, i] * inv

    pl.semaphore_wait(barrier, total)

    def one(f, a):
        ref, count = field(f)
        if a == 1:
            faces_x(f, lambda i, r: ref[1 + i, PAD + r : PAD + r + 1], count)
        if a == 2:
            pack(f, lambda i: ref[1 + i, rows], count, 2)
        send(f, a)

    one(1, 1)
    one(2, 2)
    one(0, 0)
    for f, a in ((0, 1), (2, 1), (1, 0), (2, 0), (0, 2), (1, 2)):
        one(f, a)

    loads[6].wait()
    for i in range(n0):
        NI[i] = 1.0 / (6.0 + NI[i])
    loads[7].wait()
    spread_rows = (
        lax.broadcasted_iota(jnp.int32, (n1, m1), 0) // 2 == lax.broadcasted_iota(jnp.int32, (n1, m1), 1)
    ).astype(jnp.float32)
    spread_cols = (
        lax.broadcasted_iota(jnp.int32, (m2, n2), 1) // 2 == lax.broadcasted_iota(jnp.int32, (m2, n2), 0)
    ).astype(jnp.float32)
    exact = functools.partial(
        jnp.dot, precision=lax.Precision.HIGHEST, preferred_element_type=jnp.float32
    )
    for i in range(m0):
        CI[i] = exact(spread_rows, exact(1.0 / (6.0 + CS[i]), spread_cols))

    receive(1, 1)
    rows_x(1, 1)
    receive(0, 0)
    receive(2, 2)
    ws = arrived(2, 2)
    for i in range(n0):
        x2 = S[2, 1 + i, rows]
        rhs = S[0, i, rows] - S[0, 1 + i, rows]
        rhs = rhs + (S[1, 1 + i, pl.ds(PAD - 1, n1)] - S[1, 1 + i, rows])
        rhs = rhs + (from_low(x2, halo(ws, i, 2)) - x2)
        FG[1 + i, rows] = rhs * NI[i]
    exchange(FGI, 2)

    def smooth(k):
        for a in range(3):
            if (k, a) not in ((1, 1), (0, 0), (2, 2)):
                receive(k, a)
        if k != 1:
            rows_x(k, 1)
        w = arrived(k, 2)
        for i in range(n0):
            x = S[k, 1 + i, rows]
            near = S[k, i, rows] + S[k, i + 2, rows] + inplane(S.at[k, 1 + i], x, halo(w, i, 2), 1)
            OB[k, i] = x + near * D[k, i]

    smooth(0)

    for a in range(3):
        receive(FGI, a)
    rows_x(FGI, 1)
    ws = arrived(FGI, 2)
    for c in range(m0):
        t = None
        for i in (2 * c, 2 * c + 1):
            x = FG[1 + i, rows]
            near = FG[i, rows] + FG[i + 2, rows] + inplane(FG.at[1 + i], x, halo(ws, i, 2), 1)
            F[0, i] = near
            t = near if t is None else t + near
        t = t + jnp.where(lane_full % 2 == 0, pltpu.roll(t, n2 - 1, 1), pltpu.roll(t, 1, 1))
        T[c, rows] = t
        t = t + jnp.where(row_full % 2 == 0, T[c, pl.ds(PAD + 1, n1)], T[c, pl.ds(PAD - 1, n1)])
        CR[c] = t
        V1[1 + c, rows] = t * CI[c]
    exchange(V1I, 4)

    def faces_f(j):
        f = F0I + j
        send(f, 0)
        faces_x(f, lambda i, r: F[j, i, r : r + 1], n0)
        send(f, 1)
        pack(f, lambda i: F[j, i], n0, 2)
        send(f, 2)

    for i in range(n0):
        F[0, i] = FG[1 + i, rows] + F[0, i] * NI[i]
    faces_f(0)
    smooth(1)

    for a in range(3):
        receive(V1I, a)
    rows_x(V1I, 2)
    ws1 = arrived(V1I, 4)
    for c in range(m0):
        x = V1[1 + c, rows]
        near = V1[c, rows] + V1[c + 2, rows] + inplane(V1.at[1 + c], x, halo(ws1, c, 4), 2)
        A1[c] = CR[c] - near
        V2[1 + c, rows] = x - near * CI[c]
    exchange(V2I, 4)

    def fold(x):
        acc = x[0:8]
        for g in range(1, groups):
            acc = acc + x[8 * g : 8 * g + 8]
        return acc

    def spread_near(j, V, w):
        for c in range(m0):
            x = V[1 + c, rows]
            near = x + inplane(V.at[1 + c], x, halo(w, c, 4), 1)
            F[j, 2 * c] = (near + V[c, rows]) * NI[2 * c]
            F[j, 2 * c + 1] = (near + V[c + 2, rows]) * NI[2 * c + 1]
        faces_f(j)

    sums = [jnp.zeros((8, n2), jnp.float32) for _ in range(5)]
    for c in range(m0):
        v1, v2, a1, cr = V1[1 + c, rows], V2[1 + c, rows], A1[c], CR[c]
        sums[0] = sums[0] + fold(v1 * cr)
        sums[1] = sums[1] + fold(v2 * cr)
        sums[2] = sums[2] + fold(v1 * a1)
        sums[3] = sums[3] + fold(v2 * a1)
    spread_near(1, V1, ws1)

    for a in range(3):
        receive(V2I, a)
    rows_x(V2I, 2)
    ws2 = arrived(V2I, 4)
    for c in range(m0):
        x = V2[1 + c, rows]
        near = V2[c, rows] + V2[c + 2, rows] + inplane(V2.at[1 + c], x, halo(ws2, c, 4), 2)
        sums[4] = sums[4] + fold(x * (A1[c] - near))
    part = jnp.concatenate(
        [jnp.sum(s, axis=0, keepdims=True) for s in sums] + [jnp.zeros((3, n2), jnp.float32)], axis=0
    )

    bases = (0, sizes[0], sizes[0] + sizes[1])

    def sum_message(a, slots, d):
        return pltpu.make_async_remote_copy(
            src_ref=slots.at[me[a]], dst_ref=slots.at[me[a]],
            send_sem=psend.at[bases[a] + d], recv_sem=precv.at[bases[a] + d],
            device_id={AXES[a]: lax.rem(me[a] + d, sizes[a])}, device_id_type=MESH,
        )

    def sum_start(a, slots, value):
        slots[me[a]] = value
        for d in range(1, sizes[a]):
            sum_message(a, slots, d).start()

    def sum_end(a, slots):
        for d in range(1, sizes[a]):
            src = lax.rem(me[a] + sizes[a] - d, sizes[a])
            pltpu.make_async_remote_copy(
                src_ref=slots.at[src], dst_ref=slots.at[src],
                send_sem=psend.at[bases[a] + d], recv_sem=precv.at[bases[a] + d],
                device_id={AXES[a]: src}, device_id_type=MESH,
            ).wait_recv()
        value = slots[0]
        for d in range(1, sizes[a]):
            value = value + slots[d]
        return value

    sum_start(0, PZ, part)
    part = sum_end(0, PZ)
    sum_start(1, PX, part)
    spread_near(2, V2, ws2)
    part = sum_end(1, PX)
    sum_start(2, PY, part)
    smooth(2)
    for j in range(3):
        for a in range(3):
            receive(F0I + j, a)
    part = sum_end(2, PY)
    tot = jnp.sum(part, axis=1, keepdims=True)
    gone, gtwo, hone, hmix, htwo = [tot[q : q + 1] for q in range(5)]
    two = (gtwo - hmix * gone / hone) / (htwo - hmix * hmix / hone)
    oneco = (gone - hmix * two) / hone

    def mix(get):
        a = get(0)
        return a + jnp.broadcast_to(oneco, a.shape) * get(1) + jnp.broadcast_to(two, a.shape) * get(2)

    for i in range(n0 + 1):
        FN[i, 0:n1] = mix(lambda j: F[j, i])
    for i in range(n0):
        FN[i, n1 : n1 + 1] = mix(lambda j: RX[F0I + j, 1, i : i + 1])
    wf = [mix(lambda j: RY[F0I + j, 1, v]) for v in range(RY.shape[2])]
    stores = []
    for i in range(n0):
        x = FN[i, 0:n1]
        OB[0, i] = OB[0, i] + (FN[i + 1, 0:n1] - x)
        OB[1, i] = OB[1, i] + (FN[i, 1 : n1 + 1] - x)
        OB[2, i] = OB[2, i] + (from_high(x, halo(wf, i, 2)) - x)
        if i % 4 == 3 or i == n0 - 1:
            lo = 4 * (i // 4)
            for k in range(3):
                part_of = pl.ds(lo, i + 1 - lo)
                copy = pltpu.make_async_copy(OB.at[k, part_of], out.at[k, part_of], out_sem.at[len(stores)])
                copy.start()
                stores.append(copy)

    for a, slots in ((0, PZ), (1, PX), (2, PY)):
        for d in range(1, sizes[a]):
            sum_message(a, slots, d).wait_send()
    for a in range(3):
        for d in (0, 1):
            def drain(a=a, d=d):
                for f in range(9):
                    if d in dirs(f):
                        message(f, a, d).wait_send()
            pl.when(can_send(a, d))(drain)
    for copy in stores:
        copy.wait()


def solution(mesh):
    sizes = tuple(mesh.shape[a] for a in AXES)

    def local(residual, edge_diag, node_shift, coarse_shift):
        n0, n1, n2 = node_shift.shape
        m0, m1, m2 = coarse_shift.shape
        vecs = max(-(-(n0 * (n1 // 8)) // (n2 // 2)), -(-(m0 * (n1 // 8)) // (n2 // 4)))
        f32 = jnp.float32
        V = lambda *s: pltpu.VMEM(s, f32)
        scratch = [
            V(3, n0, n1, n2), V(3, n0, n1, n2), V(n0, n1, n2), V(m0, m1, m2),
            V(3, n0 + 2, n1 + 2 * PAD, n2), V(n0 + 2, n1 + 2 * PAD, n2),
            V(m0, n1, n2), V(m0, n1, n2), V(m0, n1, n2), V(m0, n1 + 2 * PAD, n2),
            V(m0 + 2, n1 + 2 * PAD, n2), V(m0 + 2, n1 + 2 * PAD, n2),
            V(3, n0 + 1, n1, n2), V(n0 + 1, n1 + PAD, n2), V(3, n0, n1, n2),
            V(9, 2, n0, n2), V(9, 2, n0, n2), V(9, vecs, 8, n2), V(9, 2, vecs, 8, n2),
            V(sizes[0], 8, n2), V(sizes[1], 8, n2), V(sizes[2], 8, n2),
            pltpu.SemaphoreType.DMA((8,)), pltpu.SemaphoreType.DMA((3 * (-(-n0 // 4)),)),
            pltpu.SemaphoreType.DMA((9, 3, 2)), pltpu.SemaphoreType.DMA((9, 3, 2)),
            pltpu.SemaphoreType.DMA((sum(sizes),)), pltpu.SemaphoreType.DMA((sum(sizes),)),
        ]
        return pl.pallas_call(
            functools.partial(kernel, sizes),
            out_shape=jax.ShapeDtypeStruct(residual.shape, f32),
            in_specs=[pl.BlockSpec(memory_space=pl.ANY)] * 4,
            out_specs=pl.BlockSpec(memory_space=pl.ANY),
            scratch_shapes=scratch,
            compiler_params=pltpu.CompilerParams(collective_id=0, has_side_effects=True),
        )(residual, edge_diag, node_shift, coarse_shift)

    placed = (
        P(None, "gz", "gx", "gy"),
        P(None, "gz", "gx", "gy"),
        P("gz", "gx", "gy"),
        P("gz", "gx", "gy"),
    )
    return jax.shard_map(
        local, mesh=mesh, in_specs=placed, out_specs=P(None, "gz", "gx", "gy"), check_vma=False
    )
```

```python
import functools
import itertools
import math

import jax
import jax.numpy as jnp
from jax import lax
from jax.experimental import pallas as pl
from jax.experimental.pallas import tpu as pltpu
from jax.sharding import PartitionSpec as P

MESH = pl.DeviceIdType.MESH
AXES = ("gz", "gx", "gy")
FGI, V1I, V2I, F0I = 3, 4, 5, 6
PAD = 8
PHASES = ((0, 1), (2,))


def kernel(
    sizes,
    res, dia, shf, csh, OB,
    R, D, NI, CS, S, FG, CI, CR, A1, T, V1, V2, F, FN,
    SX, RX, SY, RY, PA, PB,
    in_sem, send_sem, recv_sem, psend, precv,
):
    n0, n1, n2 = NI.shape
    m0, m1, m2 = CS.shape
    groups = n1 // 8
    me = [lax.axis_index(a) for a in AXES]
    rows = pl.ds(PAD, n1)

    def offsets(axes):
        every = itertools.product(*[range(sizes[a]) for a in axes])
        return [offs for offs in every if any(offs)]

    def partner(axes, offs, sign):
        return {
            AXES[a]: lax.rem(me[a] + (o if sign > 0 else sizes[a] - o), sizes[a]) for a, o in zip(axes, offs)
        }

    loads = []
    for k in (1, 2, 0):
        for src, dst in ((res, R), (dia, D)):
            loads.append(pltpu.make_async_copy(src.at[k], dst.at[k], in_sem.at[len(loads)]))
    loads.append(pltpu.make_async_copy(shf, NI, in_sem.at[6]))
    loads.append(pltpu.make_async_copy(csh, CS, in_sem.at[7]))
    for c in loads:
        c.start()

    zplane = jnp.zeros((n1, n2), jnp.float32)
    for k in range(3):
        S[k, 0, rows] = zplane
        S[k, n0 + 1, rows] = zplane
        F[k, n0] = zplane
    FG[0, rows] = zplane
    FG[n0 + 1, rows] = zplane
    for V in (V1, V2):
        V[0, rows] = zplane
        V[m0 + 1, rows] = zplane
    RX[...] = jnp.zeros(RX.shape, jnp.float32)
    RY[...] = jnp.zeros(RY.shape, jnp.float32)
    barrier = pltpu.get_barrier_semaphore()
    total = 0
    for axes in PHASES:
        for offs in offsets(axes):
            pl.semaphore_signal(barrier, inc=1, device_id=partner(axes, offs, 1), device_id_type=MESH)
            total += 1

    lane = lax.broadcasted_iota(jnp.int32, (8, n2), 1)
    lane_full = lax.broadcasted_iota(jnp.int32, (n1, n2), 1)
    row_full = lax.broadcasted_iota(jnp.int32, (n1, n2), 0)
    row8 = lax.broadcasted_iota(jnp.int32, (8, n2), 0)
    keys = {p: ((lane + p // 2) // p) % (n2 // p) for p in (2, 4)}
    is_low = {p: (lane % p) >= p // 2 for p in (2, 4)}

    def place(i, g, p):
        k = i * groups + g
        per = n2 // p
        return k // per, k % per

    def pack(f, plane, count, p):
        accs = [jnp.zeros((8, n2), jnp.float32) for _ in range(place(count - 1, groups - 1, p)[0] + 1)]
        for i in range(count):
            x = plane(i)
            for g in range(groups):
                v, kk = place(i, g, p)
                part = x[8 * g : 8 * g + 8]
                if kk:
                    part = pltpu.roll(part, p * kk, 1)
                accs[v] = jnp.where(keys[p] == kk, part, accs[v])
        for v, acc in enumerate(accs):
            SY[f, v] = acc

    def arrived(f, p):
        return [jnp.where(is_low[p], RY[f, 0, v], RY[f, 1, v]) for v in range(RY.shape[2])]

    def halo(ws, i, p):
        parts = []
        for g in range(groups):
            v, kk = place(i, g, p)
            parts.append(pltpu.roll(ws[v], n2 - p * kk, 1) if kk else ws[v])
        return jnp.concatenate(parts, axis=0)

    def from_low(x, h, sh=1):
        return pltpu.roll(jnp.where(lane_full >= n2 - sh, h, x), sh, 1)

    def from_high(x, h, sh=1):
        return pltpu.roll(jnp.where(lane_full < sh, h, x), n2 - sh, 1)

    def inplane(ref, x, h, sh):
        near = ref[pl.ds(PAD - sh, n1)] + ref[pl.ds(PAD + sh, n1)]
        return near + from_low(x, h, sh) + from_high(x, h, sh)

    def local_near(ref, i, n, sh):
        x = ref[1 + i, rows]
        near = jnp.where(row_full >= sh, ref[1 + i, pl.ds(PAD - sh, n1)], 0.0)
        near = near + jnp.where(row_full < n1 - sh, ref[1 + i, pl.ds(PAD + sh, n1)], 0.0)
        near = near + jnp.where(lane_full >= sh, pltpu.roll(x, sh, 1), 0.0)
        near = near + jnp.where(lane_full < n2 - sh, pltpu.roll(x, n2 - sh, 1), 0.0)
        if i > 0:
            near = near + ref[i, rows]
        if i < n - 1:
            near = near + ref[i + 2, rows]
        return near

    def edges(f, p):
        sh = p // 2
        return [
            jnp.where(is_low[p], pltpu.roll(RY[f, 1, v], n2 - sh, 1), pltpu.roll(RY[f, 0, v], sh, 1))
            for v in range(RY.shape[2])
        ]

    def outer_near(near, ref, f, ws, i, n, p):
        sh = p // 2
        if i == 0:
            near = near + ref[0, rows]
        if i == n - 1:
            near = near + ref[n + 1, rows]
        side = (lane_full < sh) | (lane_full >= n2 - sh)
        near = near + jnp.where(side, halo(ws, i, p), 0.0)
        low = near[0:8] + jnp.where(row8 < sh, RX[f, 0, i : i + 1], 0.0)
        high = near[n1 - 8 : n1] + jnp.where(row8 >= 8 - sh, RX[f, 1, i : i + 1], 0.0)
        return jnp.concatenate([low, near[8 : n1 - 8], high], axis=0)

    def field(f):
        if f < 3:
            return S.at[f], n0
        return {FGI: (FG, n0), V1I: (V1, m0), V2I: (V2, m0)}[f]

    def message(f, a, d):
        if a == 0:
            if f >= F0I:
                src, dst = F.at[f - F0I, 0], F.at[f - F0I, n0]
            else:
                ref, n = field(f)
                src = ref.at[n if d else 1, rows]
                dst = ref.at[0 if d else n + 1, rows]
        elif a == 1:
            count = m0 if f in (V1I, V2I) else n0
            src, dst = SX.at[f, d, pl.ds(0, count)], RX.at[f, 1 - d, pl.ds(0, count)]
        else:
            src, dst = SY.at[f], RY.at[f, 1 - d]
        step = 1 if d else -1
        return pltpu.make_async_remote_copy(
            src_ref=src, dst_ref=dst, send_sem=send_sem.at[f, a, d], recv_sem=recv_sem.at[f, a, d],
            device_id={AXES[a]: lax.rem(me[a] + step + sizes[a], sizes[a])}, device_id_type=MESH,
        )

    def dirs(f):
        return (0,) if f >= F0I else (0, 1)

    def can_send(a, d):
        return me[a] < sizes[a] - 1 if d else me[a] > 0

    def send(f, a):
        for d in dirs(f):
            pl.when(can_send(a, d))(lambda f=f, a=a, d=d: message(f, a, d).start())

    def receive(f, a):
        for d in dirs(f):
            pl.when(can_send(a, 1 - d))(lambda f=f, a=a, d=d: message(f, a, d).wait_recv())

    def faces_x(f, get, count):
        for i in range(count):
            SX[f, 0, i : i + 1] = get(i, 0)
            if f < F0I:
                SX[f, 1, i : i + 1] = get(i, n1 - 1)

    def rows_x(f, width):
        ref, count = field(f)
        for i in range(count):
            for w in range(width):
                ref[1 + i, PAD - 1 - w : PAD - w] = RX[f, 0, i : i + 1]
                ref[1 + i, PAD + n1 + w : PAD + n1 + w + 1] = RX[f, 1, i : i + 1]

    def exchange(f, p):
        ref, count = field(f)
        send(f, 0)
        faces_x(f, lambda i, r: ref[1 + i, PAD + r : PAD + r + 1], count)
        send(f, 1)
        pack(f, lambda i: ref[1 + i, rows], count, p)
        send(f, 2)

    def one(f, a):
        ref, count = field(f)
        if a == 1:
            faces_x(f, lambda i, r: ref[1 + i, PAD + r : PAD + r + 1], count)
        if a == 2:
            pack(f, lambda i: ref[1 + i, rows], count, 2)
        send(f, a)

    for pos, (k, a) in enumerate(((1, 1), (2, 2), (0, 0))):
        loads[2 * pos].wait()
        loads[2 * pos + 1].wait()
        for i in range(n0):
            inv = 1.0 / D[k, i]
            D[k, i] = inv
            S[k, 1 + i, rows] = R[k, i] * inv
        if pos == 0:
            pl.semaphore_wait(barrier, total)
        one(k, a)
    for f, a in ((0, 1), (2, 1), (1, 0), (2, 0), (0, 2), (1, 2)):
        one(f, a)

    loads[6].wait()
    for i in range(n0):
        NI[i] = 1.0 / (6.0 + NI[i])
    loads[7].wait()
    spread_rows = (
        lax.broadcasted_iota(jnp.int32, (n1, m1), 0) // 2 == lax.broadcasted_iota(jnp.int32, (n1, m1), 1)
    ).astype(jnp.float32)
    spread_cols = (
        lax.broadcasted_iota(jnp.int32, (m2, n2), 1) // 2 == lax.broadcasted_iota(jnp.int32, (m2, n2), 0)
    ).astype(jnp.float32)
    exact = functools.partial(
        jnp.dot, precision=lax.Precision.HIGHEST, preferred_element_type=jnp.float32
    )
    for i in range(m0):
        CI[i] = exact(spread_rows, exact(1.0 / (6.0 + CS[i]), spread_cols))

    for i in range(n0):
        x1, x2 = S[1, 1 + i, rows], S[2, 1 + i, rows]
        rhs = jnp.where(row_full >= 1, S[1, 1 + i, pl.ds(PAD - 1, n1)], 0.0) - x1
        rhs = rhs + (jnp.where(lane_full >= 1, pltpu.roll(x2, 1, 1), 0.0) - x2)
        rhs = rhs - S[0, 1 + i, rows]
        if i > 0:
            rhs = rhs + S[0, i, rows]
        F[0, i] = rhs
    receive(1, 1)
    receive(0, 0)
    receive(2, 2)
    ws = edges(2, 2)
    for i in range(n0):
        rhs = F[0, i] + jnp.where(lane_full < 1, halo(ws, i, 2), 0.0)
        if i == 0:
            rhs = rhs + S[0, 0, rows]
        first = rhs[0:8] + jnp.where(row8 < 1, RX[1, 0, i : i + 1], 0.0)
        FG[1 + i, rows] = jnp.concatenate([first, rhs[8:]], axis=0) * NI[i]
    exchange(FGI, 2)

    def smooth(k):
        for a in range(3):
            if (k, a) not in ((1, 1), (0, 0), (2, 2)):
                receive(k, a)
        rows_x(k, 1)
        w = arrived(k, 2)
        for i in range(n0):
            x = S[k, 1 + i, rows]
            near = S[k, i, rows] + S[k, i + 2, rows] + inplane(S.at[k, 1 + i], x, halo(w, i, 2), 1)
            OB[k, i] = x + near * D[k, i]

    for i in range(n0):
        F[0, i] = local_near(FG, i, n0, 1)
    smooth(0)

    for a in range(3):
        receive(FGI, a)
    ws = edges(FGI, 2)
    for c in range(m0):
        t = None
        for i in (2 * c, 2 * c + 1):
            near = outer_near(F[0, i], FG, FGI, ws, i, n0, 2)
            F[0, i] = near
            t = near if t is None else t + near
        t = t + jnp.where(lane_full % 2 == 0, pltpu.roll(t, n2 - 1, 1), pltpu.roll(t, 1, 1))
        T[c, rows] = t
        t = t + jnp.where(row_full % 2 == 0, T[c, pl.ds(PAD + 1, n1)], T[c, pl.ds(PAD - 1, n1)])
        CR[c] = t
        V1[1 + c, rows] = t * CI[c]
    exchange(V1I, 4)
    for c in range(m0):
        A1[c] = local_near(V1, c, m0, 2)

    def faces_f(j):
        f = F0I + j
        send(f, 0)
        faces_x(f, lambda i, r: F[j, i, r : r + 1], n0)
        send(f, 1)
        pack(f, lambda i: F[j, i], n0, 2)
        send(f, 2)

    for i in range(n0):
        F[0, i] = FG[1 + i, rows] + F[0, i] * NI[i]
    faces_f(0)
    smooth(1)

    for a in range(3):
        receive(V1I, a)
    ws = edges(V1I, 4)
    for c in range(m0):
        near = outer_near(A1[c], V1, V1I, ws, c, m0, 4)
        A1[c] = CR[c] - near
        V2[1 + c, rows] = V1[1 + c, rows] - near * CI[c]
    exchange(V2I, 4)

    def fold(x):
        acc = x[0:8]
        for g in range(1, groups):
            acc = acc + x[8 * g : 8 * g + 8]
        return acc

    def spread_near(j, V, w):
        for c in range(m0):
            x = V[1 + c, rows]
            near = x + inplane(V.at[1 + c], x, halo(w, c, 4), 1)
            F[j, 2 * c] = (near + V[c, rows]) * NI[2 * c]
            F[j, 2 * c + 1] = (near + V[c + 2, rows]) * NI[2 * c + 1]
        faces_f(j)

    sums = [jnp.zeros((8, n2), jnp.float32) for _ in range(5)]
    for c in range(m0):
        v1, v2, a1, cr = V1[1 + c, rows], V2[1 + c, rows], A1[c], CR[c]
        sums[0] = sums[0] + fold(v1 * cr)
        sums[1] = sums[1] + fold(v2 * cr)
        sums[2] = sums[2] + fold(v1 * a1)
        sums[3] = sums[3] + fold(v2 * a1)
        sums[4] = sums[4] + fold(v2 * (a1 - local_near(V2, c, m0, 2)))
    rows_x(V1I, 2)
    spread_near(1, V1, arrived(V1I, 4))

    for a in range(3):
        receive(V2I, a)
    outer = fold(V2[1, rows] * V2[0, rows] + V2[m0, rows] * V2[m0 + 1, rows])
    for v, w in enumerate(edges(V2I, 4)):
        outer = outer + SY[V2I, v] * w
    rim = SX[V2I, 0, 0:m0] * RX[V2I, 0, 0:m0] + SX[V2I, 1, 0:m0] * RX[V2I, 1, 0:m0]
    sums[4] = sums[4] - outer
    rim = 2.0 * jnp.sum(rim, axis=0, keepdims=True)
    sums[4] = sums[4] - jnp.where(row8 == 0, rim, 0.0)
    part = jnp.concatenate(
        [jnp.sum(s, axis=0, keepdims=True) for s in sums] + [jnp.zeros((3, n2), jnp.float32)], axis=0
    )

    def slot(axes, at):
        index = 0
        for a in axes:
            index = index * sizes[a] + at(a)
        return index

    def sum_message(p, offs, sign):
        axes, slots = PHASES[p], (PA, PB)[p]
        other = partner(axes, offs, sign)
        index = slot(axes, (lambda a: me[a]) if sign > 0 else (lambda a: other[AXES[a]]))
        sem = p * PA.shape[0] + slot(axes, lambda a: offs[axes.index(a)])
        return pltpu.make_async_remote_copy(
            src_ref=slots.at[index], dst_ref=slots.at[index], send_sem=psend.at[sem], recv_sem=precv.at[sem],
            device_id=other, device_id_type=MESH,
        )

    def sum_start(p, value):
        (PA, PB)[p][slot(PHASES[p], lambda a: me[a])] = value
        for offs in offsets(PHASES[p]):
            sum_message(p, offs, 1).start()

    def sum_end(p):
        for offs in offsets(PHASES[p]):
            sum_message(p, offs, -1).wait_recv()
        slots = (PA, PB)[p]
        return functools.reduce(lambda x, y: x + y, [slots[d] for d in range(slots.shape[0])])

    sum_start(0, part)
    rows_x(V2I, 2)
    spread_near(2, V2, arrived(V2I, 4))
    part = sum_end(0)
    sum_start(1, part)
    smooth(2)
    for j in range(3):
        for a in range(3):
            receive(F0I + j, a)
    part = sum_end(1)
    tot = jnp.sum(part, axis=1, keepdims=True)
    gone, gtwo, hone, hmix, htwo = [tot[q : q + 1] for q in range(5)]
    two = (gtwo - hmix * gone / hone) / (htwo - hmix * hmix / hone)
    oneco = (gone - hmix * two) / hone

    def mix(get):
        a = get(0)
        return a + jnp.broadcast_to(oneco, a.shape) * get(1) + jnp.broadcast_to(two, a.shape) * get(2)

    for i in range(n0 + 1):
        FN[i, 0:n1] = mix(lambda j: F[j, i])
    for i in range(n0):
        FN[i, n1 : n1 + 1] = mix(lambda j: RX[F0I + j, 1, i : i + 1])
    wf = [mix(lambda j: RY[F0I + j, 1, v]) for v in range(RY.shape[2])]
    for i in range(n0):
        x = FN[i, 0:n1]
        OB[0, i] = OB[0, i] + (FN[i + 1, 0:n1] - x)
        OB[1, i] = OB[1, i] + (FN[i, 1 : n1 + 1] - x)
        OB[2, i] = OB[2, i] + (from_high(x, halo(wf, i, 2)) - x)

    for p in (0, 1):
        for offs in offsets(PHASES[p]):
            sum_message(p, offs, 1).wait_send()
    for a in range(3):
        for d in (0, 1):
            def drain(a=a, d=d):
                for f in range(9):
                    if d in dirs(f):
                        message(f, a, d).wait_send()
            pl.when(can_send(a, d))(drain)


def solution(mesh):
    sizes = tuple(mesh.shape[a] for a in AXES)

    def local(residual, edge_diag, node_shift, coarse_shift):
        n0, n1, n2 = node_shift.shape
        m0, m1, m2 = coarse_shift.shape
        vecs = max(-(-(n0 * (n1 // 8)) // (n2 // 2)), -(-(m0 * (n1 // 8)) // (n2 // 4)))
        f32 = jnp.float32
        counts = [math.prod(sizes[a] for a in axes) for axes in PHASES]
        V = lambda *s: pltpu.VMEM(s, f32)
        scratch = [
            V(3, n0, n1, n2), V(3, n0, n1, n2), V(n0, n1, n2), V(m0, m1, m2),
            V(3, n0 + 2, n1 + 2 * PAD, n2), V(n0 + 2, n1 + 2 * PAD, n2),
            V(m0, n1, n2), V(m0, n1, n2), V(m0, n1, n2), V(m0, n1 + 2 * PAD, n2),
            V(m0 + 2, n1 + 2 * PAD, n2), V(m0 + 2, n1 + 2 * PAD, n2),
            V(3, n0 + 1, n1, n2), V(n0 + 1, n1 + PAD, n2),
            V(9, 2, n0, n2), V(9, 2, n0, n2), V(9, vecs, 8, n2), V(9, 2, vecs, 8, n2),
            *[V(c, 8, n2) for c in counts],
            pltpu.SemaphoreType.DMA((8,)),
            pltpu.SemaphoreType.DMA((9, 3, 2)), pltpu.SemaphoreType.DMA((9, 3, 2)),
            pltpu.SemaphoreType.DMA((sum(counts),)), pltpu.SemaphoreType.DMA((sum(counts),)),
        ]
        limit = 67_043_328 - 4 * math.prod(residual.shape) - 2**16
        return pl.pallas_call(
            functools.partial(kernel, sizes),
            out_shape=pltpu.VMEM(residual.shape, f32),
            in_specs=[pl.BlockSpec(memory_space=pltpu.HBM)] * 4,
            out_specs=pl.BlockSpec(memory_space=pltpu.VMEM),
            scratch_shapes=scratch,
            compiler_params=pltpu.CompilerParams(collective_id=0, has_side_effects=True, vmem_limit_bytes=limit),
        )(residual, edge_diag, node_shift, coarse_shift)

    placed = (
        P(None, "gz", "gx", "gy"),
        P(None, "gz", "gx", "gy"),
        P("gz", "gx", "gy"),
        P("gz", "gx", "gy"),
    )
    return jax.shard_map(
        local, mesh=mesh, in_specs=placed, out_specs=P(None, "gz", "gx", "gy"), check_vma=False
    )
```

```python
import functools
import itertools
import math

import jax
import jax.numpy as jnp
from jax import lax
from jax.experimental import pallas as pl
from jax.experimental.pallas import tpu as pltpu
from jax.sharding import PartitionSpec as P

MESH = pl.DeviceIdType.MESH
AXES = ("gz", "gx", "gy")
FGI, V1I, V2I, F0I = 3, 4, 5, 6
PAD = 8
PHASES = ((1, 2), (0,))


def kernel(
    sizes,
    res, dia, shf, csh, OB,
    R, D, NI, CS, S, FG, CI, CR, A1, T, V1, V2, F, FN,
    SX, RX, SY, RY, PA, PB,
    in_sem, send_sem, recv_sem, psend, precv,
):
    n0, n1, n2 = NI.shape
    m0, m1, m2 = CS.shape
    groups = n1 // 8
    me = [lax.axis_index(a) for a in AXES]
    rows = pl.ds(PAD, n1)

    def offsets(axes):
        every = itertools.product(*[range(sizes[a]) for a in axes])
        return [offs for offs in every if any(offs)]

    def partner(axes, offs, sign):
        return {
            AXES[a]: lax.rem(me[a] + (o if sign > 0 else sizes[a] - o), sizes[a]) for a, o in zip(axes, offs)
        }

    loads = []
    for k in (1, 2, 0):
        for src, dst in ((res, R), (dia, D)):
            loads.append(pltpu.make_async_copy(src.at[k], dst.at[k], in_sem.at[len(loads)]))
    loads.append(pltpu.make_async_copy(shf, NI, in_sem.at[6]))
    loads.append(pltpu.make_async_copy(csh, CS, in_sem.at[7]))
    for c in loads:
        c.start()

    zplane = jnp.zeros((n1, n2), jnp.float32)
    for k in range(3):
        S[k, 0, rows] = zplane
        S[k, n0 + 1, rows] = zplane
        F[k, n0] = zplane
    FG[0, rows] = zplane
    FG[n0 + 1, rows] = zplane
    for V in (V1, V2):
        V[0, rows] = zplane
        V[m0 + 1, rows] = zplane
    RX[...] = jnp.zeros(RX.shape, jnp.float32)
    RY[...] = jnp.zeros(RY.shape, jnp.float32)
    barrier = pltpu.get_barrier_semaphore()
    total = 0
    for axes in PHASES:
        for offs in offsets(axes):
            pl.semaphore_signal(barrier, inc=1, device_id=partner(axes, offs, 1), device_id_type=MESH)
            total += 1

    lane = lax.broadcasted_iota(jnp.int32, (8, n2), 1)
    lane_full = lax.broadcasted_iota(jnp.int32, (n1, n2), 1)
    row_full = lax.broadcasted_iota(jnp.int32, (n1, n2), 0)
    row8 = lax.broadcasted_iota(jnp.int32, (8, n2), 0)
    keys = {p: ((lane + p // 2) // p) % (n2 // p) for p in (2, 4)}
    is_low = {p: (lane % p) >= p // 2 for p in (2, 4)}

    def place(i, g, p):
        k = i * groups + g
        per = n2 // p
        return k // per, k % per

    def pack(f, plane, count, p):
        accs = [jnp.zeros((8, n2), jnp.float32) for _ in range(place(count - 1, groups - 1, p)[0] + 1)]
        for i in range(count):
            x = plane(i)
            for g in range(groups):
                v, kk = place(i, g, p)
                part = x[8 * g : 8 * g + 8]
                if kk:
                    part = pltpu.roll(part, p * kk, 1)
                accs[v] = jnp.where(keys[p] == kk, part, accs[v])
        for v, acc in enumerate(accs):
            SY[f, v] = acc

    def arrived(f, p):
        return [jnp.where(is_low[p], RY[f, 0, v], RY[f, 1, v]) for v in range(RY.shape[2])]

    def halo(ws, i, p):
        parts = []
        for g in range(groups):
            v, kk = place(i, g, p)
            parts.append(pltpu.roll(ws[v], n2 - p * kk, 1) if kk else ws[v])
        return jnp.concatenate(parts, axis=0)

    def from_low(x, h, sh=1):
        return pltpu.roll(jnp.where(lane_full >= n2 - sh, h, x), sh, 1)

    def from_high(x, h, sh=1):
        return pltpu.roll(jnp.where(lane_full < sh, h, x), n2 - sh, 1)

    def inplane(ref, x, h, sh):
        near = ref[pl.ds(PAD - sh, n1)] + ref[pl.ds(PAD + sh, n1)]
        return near + from_low(x, h, sh) + from_high(x, h, sh)

    def local_near(ref, i, n, sh):
        x = ref[1 + i, rows]
        near = jnp.where(row_full >= sh, ref[1 + i, pl.ds(PAD - sh, n1)], 0.0)
        near = near + jnp.where(row_full < n1 - sh, ref[1 + i, pl.ds(PAD + sh, n1)], 0.0)
        near = near + jnp.where(lane_full >= sh, pltpu.roll(x, sh, 1), 0.0)
        near = near + jnp.where(lane_full < n2 - sh, pltpu.roll(x, n2 - sh, 1), 0.0)
        if i > 0:
            near = near + ref[i, rows]
        if i < n - 1:
            near = near + ref[i + 2, rows]
        return near

    def edges(f, p):
        sh = p // 2
        return [
            jnp.where(is_low[p], pltpu.roll(RY[f, 1, v], n2 - sh, 1), pltpu.roll(RY[f, 0, v], sh, 1))
            for v in range(RY.shape[2])
        ]

    def outer_near(near, ref, f, ws, i, n, p):
        sh = p // 2
        if i == 0:
            near = near + ref[0, rows]
        if i == n - 1:
            near = near + ref[n + 1, rows]
        side = (lane_full < sh) | (lane_full >= n2 - sh)
        near = near + jnp.where(side, halo(ws, i, p), 0.0)
        low = near[0:8] + jnp.where(row8 < sh, RX[f, 0, i : i + 1], 0.0)
        high = near[n1 - 8 : n1] + jnp.where(row8 >= 8 - sh, RX[f, 1, i : i + 1], 0.0)
        return jnp.concatenate([low, near[8 : n1 - 8], high], axis=0)

    def field(f):
        if f < 3:
            return S.at[f], n0
        return {FGI: (FG, n0), V1I: (V1, m0), V2I: (V2, m0)}[f]

    def message(f, a, d):
        if a == 0:
            if f >= F0I:
                src, dst = F.at[f - F0I, 0], F.at[f - F0I, n0]
            else:
                ref, n = field(f)
                src = ref.at[n if d else 1, rows]
                dst = ref.at[0 if d else n + 1, rows]
        elif a == 1:
            count = m0 if f in (V1I, V2I) else n0
            src, dst = SX.at[f, d, pl.ds(0, count)], RX.at[f, 1 - d, pl.ds(0, count)]
        else:
            src, dst = SY.at[f], RY.at[f, 1 - d]
        step = 1 if d else -1
        return pltpu.make_async_remote_copy(
            src_ref=src, dst_ref=dst, send_sem=send_sem.at[f, a, d], recv_sem=recv_sem.at[f, a, d],
            device_id={AXES[a]: lax.rem(me[a] + step + sizes[a], sizes[a])}, device_id_type=MESH,
        )

    def dirs(f):
        return (0,) if f >= F0I else (0, 1)

    def can_send(a, d):
        return me[a] < sizes[a] - 1 if d else me[a] > 0

    def send(f, a):
        for d in dirs(f):
            pl.when(can_send(a, d))(lambda f=f, a=a, d=d: message(f, a, d).start())

    def receive(f, a):
        for d in dirs(f):
            pl.when(can_send(a, 1 - d))(lambda f=f, a=a, d=d: message(f, a, d).wait_recv())

    def faces_x(f, get, count):
        for i in range(count):
            SX[f, 0, i : i + 1] = get(i, 0)
            if f < F0I:
                SX[f, 1, i : i + 1] = get(i, n1 - 1)

    def rows_x(f, width):
        ref, count = field(f)
        for i in range(count):
            for w in range(width):
                ref[1 + i, PAD - 1 - w : PAD - w] = RX[f, 0, i : i + 1]
                ref[1 + i, PAD + n1 + w : PAD + n1 + w + 1] = RX[f, 1, i : i + 1]

    def exchange(f, p):
        ref, count = field(f)
        send(f, 0)
        faces_x(f, lambda i, r: ref[1 + i, PAD + r : PAD + r + 1], count)
        send(f, 1)
        pack(f, lambda i: ref[1 + i, rows], count, p)
        send(f, 2)

    def one(f, a):
        ref, count = field(f)
        if a == 1:
            faces_x(f, lambda i, r: ref[1 + i, PAD + r : PAD + r + 1], count)
        if a == 2:
            pack(f, lambda i: ref[1 + i, rows], count, 2)
        send(f, a)

    for pos, (k, a) in enumerate(((1, 1), (2, 2), (0, 0))):
        loads[2 * pos].wait()
        loads[2 * pos + 1].wait()
        for i in range(n0):
            inv = 1.0 / D[k, i]
            D[k, i] = inv
            S[k, 1 + i, rows] = R[k, i] * inv
        if pos == 0:
            pl.semaphore_wait(barrier, total)
        one(k, a)
    for f, a in ((0, 1), (2, 1), (1, 0), (2, 0), (0, 2), (1, 2)):
        one(f, a)

    loads[6].wait()
    for i in range(n0):
        NI[i] = 1.0 / (6.0 + NI[i])
    loads[7].wait()
    spread_rows = (
        lax.broadcasted_iota(jnp.int32, (n1, m1), 0) // 2 == lax.broadcasted_iota(jnp.int32, (n1, m1), 1)
    ).astype(jnp.float32)
    spread_cols = (
        lax.broadcasted_iota(jnp.int32, (m2, n2), 1) // 2 == lax.broadcasted_iota(jnp.int32, (m2, n2), 0)
    ).astype(jnp.float32)
    exact = functools.partial(
        jnp.dot, precision=lax.Precision.HIGHEST, preferred_element_type=jnp.float32
    )
    for i in range(m0):
        CI[i] = exact(spread_rows, exact(1.0 / (6.0 + CS[i]), spread_cols))

    for i in range(n0):
        x1, x2 = S[1, 1 + i, rows], S[2, 1 + i, rows]
        rhs = jnp.where(row_full >= 1, S[1, 1 + i, pl.ds(PAD - 1, n1)], 0.0) - x1
        rhs = rhs + (jnp.where(lane_full >= 1, pltpu.roll(x2, 1, 1), 0.0) - x2)
        rhs = rhs - S[0, 1 + i, rows]
        if i > 0:
            rhs = rhs + S[0, i, rows]
        F[0, i] = rhs
    receive(1, 1)
    receive(0, 0)
    receive(2, 2)
    ws = edges(2, 2)
    for i in range(n0):
        rhs = F[0, i] + jnp.where(lane_full < 1, halo(ws, i, 2), 0.0)
        if i == 0:
            rhs = rhs + S[0, 0, rows]
        first = rhs[0:8] + jnp.where(row8 < 1, RX[1, 0, i : i + 1], 0.0)
        FG[1 + i, rows] = jnp.concatenate([first, rhs[8:]], axis=0) * NI[i]
    exchange(FGI, 2)

    def smooth(k):
        for a in range(3):
            if (k, a) not in ((1, 1), (0, 0), (2, 2)):
                receive(k, a)
        rows_x(k, 1)
        w = arrived(k, 2)
        for i in range(n0):
            x = S[k, 1 + i, rows]
            near = S[k, i, rows] + S[k, i + 2, rows] + inplane(S.at[k, 1 + i], x, halo(w, i, 2), 1)
            OB[k, i] = x + near * D[k, i]

    for i in range(n0):
        F[0, i] = local_near(FG, i, n0, 1)
    smooth(0)

    for a in range(3):
        receive(FGI, a)
    ws = edges(FGI, 2)
    for c in range(m0):
        t = None
        for i in (2 * c, 2 * c + 1):
            near = outer_near(F[0, i], FG, FGI, ws, i, n0, 2)
            F[0, i] = near
            t = near if t is None else t + near
        t = t + jnp.where(lane_full % 2 == 0, pltpu.roll(t, n2 - 1, 1), pltpu.roll(t, 1, 1))
        T[c, rows] = t
        t = t + jnp.where(row_full % 2 == 0, T[c, pl.ds(PAD + 1, n1)], T[c, pl.ds(PAD - 1, n1)])
        CR[c] = t
        V1[1 + c, rows] = t * CI[c]
    exchange(V1I, 4)
    for c in range(m0):
        A1[c] = local_near(V1, c, m0, 2)

    def faces_f(j):
        f = F0I + j
        send(f, 0)
        faces_x(f, lambda i, r: F[j, i, r : r + 1], n0)
        send(f, 1)
        pack(f, lambda i: F[j, i], n0, 2)
        send(f, 2)

    for i in range(n0):
        F[0, i] = FG[1 + i, rows] + F[0, i] * NI[i]
    faces_f(0)
    smooth(1)

    for a in range(3):
        receive(V1I, a)
    ws = edges(V1I, 4)
    for c in range(m0):
        near = outer_near(A1[c], V1, V1I, ws, c, m0, 4)
        A1[c] = CR[c] - near
        V2[1 + c, rows] = V1[1 + c, rows] - near * CI[c]
    exchange(V2I, 4)

    def fold(x):
        acc = x[0:8]
        for g in range(1, groups):
            acc = acc + x[8 * g : 8 * g + 8]
        return acc

    def spread_near(j, V, w):
        for c in range(m0):
            x = V[1 + c, rows]
            near = x + inplane(V.at[1 + c], x, halo(w, c, 4), 1)
            F[j, 2 * c] = (near + V[c, rows]) * NI[2 * c]
            F[j, 2 * c + 1] = (near + V[c + 2, rows]) * NI[2 * c + 1]
        faces_f(j)

    sums = [jnp.zeros((8, n2), jnp.float32) for _ in range(5)]
    for c in range(m0):
        v1, v2, a1, cr = V1[1 + c, rows], V2[1 + c, rows], A1[c], CR[c]
        sums[0] = sums[0] + fold(v1 * cr)
        sums[1] = sums[1] + fold(v2 * cr)
        sums[2] = sums[2] + fold(v1 * a1)
        sums[3] = sums[3] + fold(v2 * a1)
        sums[4] = sums[4] + fold(v2 * (a1 - local_near(V2, c, m0, 2)))
    rows_x(V1I, 2)
    spread_near(1, V1, arrived(V1I, 4))

    for a in range(3):
        receive(V2I, a)
    outer = fold(V2[1, rows] * V2[0, rows] + V2[m0, rows] * V2[m0 + 1, rows])
    for v, w in enumerate(edges(V2I, 4)):
        outer = outer + SY[V2I, v] * w
    rim = SX[V2I, 0, 0:m0] * RX[V2I, 0, 0:m0] + SX[V2I, 1, 0:m0] * RX[V2I, 1, 0:m0]
    sums[4] = sums[4] - outer
    rim = 2.0 * jnp.sum(rim, axis=0, keepdims=True)
    sums[4] = sums[4] - jnp.where(row8 == 0, rim, 0.0)
    part = jnp.concatenate(
        [jnp.sum(s, axis=0, keepdims=True) for s in sums] + [jnp.zeros((3, n2), jnp.float32)], axis=0
    )

    def slot(axes, at):
        index = 0
        for a in axes:
            index = index * sizes[a] + at(a)
        return index

    def sum_message(p, offs, sign):
        axes, slots = PHASES[p], (PA, PB)[p]
        other = partner(axes, offs, sign)
        index = slot(axes, (lambda a: me[a]) if sign > 0 else (lambda a: other[AXES[a]]))
        sem = p * PA.shape[0] + slot(axes, lambda a: offs[axes.index(a)])
        return pltpu.make_async_remote_copy(
            src_ref=slots.at[index], dst_ref=slots.at[index], send_sem=psend.at[sem], recv_sem=precv.at[sem],
            device_id=other, device_id_type=MESH,
        )

    def sum_start(p, value):
        (PA, PB)[p][slot(PHASES[p], lambda a: me[a])] = value
        for offs in offsets(PHASES[p]):
            sum_message(p, offs, 1).start()

    def sum_end(p):
        for offs in offsets(PHASES[p]):
            sum_message(p, offs, -1).wait_recv()
        slots = (PA, PB)[p]
        return functools.reduce(lambda x, y: x + y, [slots[d] for d in range(slots.shape[0])])

    sum_start(0, part)
    rows_x(V2I, 2)
    spread_near(2, V2, arrived(V2I, 4))
    smooth(2)
    part = sum_end(0)
    sum_start(1, part)
    for j in range(3):
        for a in range(3):
            receive(F0I + j, a)
    part = sum_end(1)
    tot = jnp.sum(part, axis=1, keepdims=True)
    gone, gtwo, hone, hmix, htwo = [tot[q : q + 1] for q in range(5)]
    two = (gtwo - hmix * gone / hone) / (htwo - hmix * hmix / hone)
    oneco = (gone - hmix * two) / hone

    def mix(get):
        a = get(0)
        return a + jnp.broadcast_to(oneco, a.shape) * get(1) + jnp.broadcast_to(two, a.shape) * get(2)

    for i in range(n0 + 1):
        FN[i, 0:n1] = mix(lambda j: F[j, i])
    for i in range(n0):
        FN[i, n1 : n1 + 1] = mix(lambda j: RX[F0I + j, 1, i : i + 1])
    wf = [mix(lambda j: RY[F0I + j, 1, v]) for v in range(RY.shape[2])]
    for i in range(n0):
        x = FN[i, 0:n1]
        OB[0, i] = OB[0, i] + (FN[i + 1, 0:n1] - x)
        OB[1, i] = OB[1, i] + (FN[i, 1 : n1 + 1] - x)
        OB[2, i] = OB[2, i] + (from_high(x, halo(wf, i, 2)) - x)

    for p in (0, 1):
        for offs in offsets(PHASES[p]):
            sum_message(p, offs, 1).wait_send()
    for a in range(3):
        for d in (0, 1):
            def drain(a=a, d=d):
                for f in range(9):
                    if d in dirs(f):
                        message(f, a, d).wait_send()
            pl.when(can_send(a, d))(drain)


def solution(mesh):
    sizes = tuple(mesh.shape[a] for a in AXES)

    def local(residual, edge_diag, node_shift, coarse_shift):
        n0, n1, n2 = node_shift.shape
        m0, m1, m2 = coarse_shift.shape
        vecs = max(-(-(n0 * (n1 // 8)) // (n2 // 2)), -(-(m0 * (n1 // 8)) // (n2 // 4)))
        f32 = jnp.float32
        counts = [math.prod(sizes[a] for a in axes) for axes in PHASES]
        V = lambda *s: pltpu.VMEM(s, f32)
        scratch = [
            V(3, n0, n1, n2), V(3, n0, n1, n2), V(n0, n1, n2), V(m0, m1, m2),
            V(3, n0 + 2, n1 + 2 * PAD, n2), V(n0 + 2, n1 + 2 * PAD, n2),
            V(m0, n1, n2), V(m0, n1, n2), V(m0, n1, n2), V(m0, n1 + 2 * PAD, n2),
            V(m0 + 2, n1 + 2 * PAD, n2), V(m0 + 2, n1 + 2 * PAD, n2),
            V(3, n0 + 1, n1, n2), V(n0 + 1, n1 + PAD, n2),
            V(9, 2, n0, n2), V(9, 2, n0, n2), V(9, vecs, 8, n2), V(9, 2, vecs, 8, n2),
            *[V(c, 8, n2) for c in counts],
            pltpu.SemaphoreType.DMA((8,)),
            pltpu.SemaphoreType.DMA((9, 3, 2)), pltpu.SemaphoreType.DMA((9, 3, 2)),
            pltpu.SemaphoreType.DMA((sum(counts),)), pltpu.SemaphoreType.DMA((sum(counts),)),
        ]
        limit = 67_043_328 - 4 * math.prod(residual.shape) - 2**16
        return pl.pallas_call(
            functools.partial(kernel, sizes),
            out_shape=pltpu.VMEM(residual.shape, f32),
            in_specs=[pl.BlockSpec(memory_space=pltpu.HBM)] * 4,
            out_specs=pl.BlockSpec(memory_space=pltpu.VMEM),
            scratch_shapes=scratch,
            compiler_params=pltpu.CompilerParams(collective_id=0, has_side_effects=True, vmem_limit_bytes=limit),
        )(residual, edge_diag, node_shift, coarse_shift)

    placed = (
        P(None, "gz", "gx", "gy"),
        P(None, "gz", "gx", "gy"),
        P("gz", "gx", "gy"),
        P("gz", "gx", "gy"),
    )
    return jax.shard_map(
        local, mesh=mesh, in_specs=placed, out_specs=P(None, "gz", "gx", "gy"), check_vma=False
    )
```
